16 devices in a mesh: data: 4 (over z, y), model: 4 (over x, core).
Axes of the slice: x: 2, y: 2, z: 2, core: 2. Of those that a mesh axis runs over, the one named last changes fastest.
Arguments:
- hidden: bfloat16 [8192, 2560], P('data')
- w_vocab: bfloat16 [50304, 2560], P(('model', 'data'))
- labels: int32 [8192], P('data')
- mask: int32 [8192], P('data')
Outputs:
- output 1: float32 [], replicated
- output 2: bfloat16 [8192, 2560], P('data')
- output 3: bfloat16 [50304, 2560], P(('model', 'data'))
All inputs are finite; a program needn't handle non-finite values.
Results may differ from the reference program's by a relative error of at most 0.001.
Values are sent between devices in bfloat16 or wider.
A program may use at most 1 GiB of HBM per device.

```python
import jax
import jax.numpy as jnp
from jax import lax

VOCAB_SIZE = 50304
MODEL_DIM = 2560
NUM_TOKENS = 8192
ROW_BLOCK = 256


def draw_targets(perm_key, offset_key, length_key):
    bin_width = VOCAB_SIZE // 128
    tok_perm = jax.random.permutation(perm_key, NUM_TOKENS)
    coarse_bin = (tok_perm * 128) // NUM_TOKENS
    bin_offset = jax.random.randint(offset_key, (NUM_TOKENS,), 0, bin_width)
    labels = coarse_bin * bin_width + bin_offset
    labels = jnp.where(tok_perm == 0, 0, labels)
    labels = jnp.where(tok_perm == NUM_TOKENS - 1, VOCAB_SIZE - 1, labels)
    group_len = jax.random.randint(length_key, (NUM_TOKENS // 32, 1), 1, 33)
    position = jnp.arange(32, dtype=jnp.int32)[None, :]
    mask = (position < group_len).astype(jnp.int32).reshape(NUM_TOKENS)
    return labels.astype(jnp.int32), mask


def setup_inputs(seed: int = 0) -> dict:
    root_key = jax.random.key(seed)
    hid_key, weight_key, perm_key, offset_key, length_key = jax.random.split(root_key, 5)
    hidden = jax.random.normal(hid_key, (NUM_TOKENS, MODEL_DIM), jnp.float32).astype(jnp.bfloat16)
    w_scale = 3.0 / MODEL_DIM ** 0.5
    w_vocab = (jax.random.normal(weight_key, (VOCAB_SIZE, MODEL_DIM), jnp.float32) * w_scale).astype(jnp.bfloat16)
    labels, mask = draw_targets(perm_key, offset_key, length_key)
    return {"hidden": hidden, "w_vocab": w_vocab, "labels": labels, "mask": mask}


def reference(hidden, w_vocab, labels, mask):
    weight = mask.astype(jnp.float32)
    token_count = jnp.sum(weight)
    vocab_ids = jnp.arange(VOCAB_SIZE, dtype=jnp.int32)
    block_count = NUM_TOKENS // ROW_BLOCK
    hid_blocks = hidden.reshape(block_count, ROW_BLOCK, MODEL_DIM)
    lab_blocks = labels.reshape(block_count, ROW_BLOCK)
    wgt_blocks = weight.reshape(block_count, ROW_BLOCK)

    def step(carry, block):
        loss_sum, dw_acc = carry
        hid_rows, lab_rows, wgt_rows = block
        logits = lax.dot_general(hid_rows, w_vocab, (((1,), (1,)), ((), ())), preferred_element_type=jnp.float32)
        row_max = jnp.max(logits, axis=1)
        exp_shift = jnp.exp(logits - row_max[:, None])
        sum_exp = jnp.sum(exp_shift, axis=1)
        log_norm = row_max + jnp.log(sum_exp)
        is_target = vocab_ids[None, :] == lab_rows[:, None]
        target = jnp.sum(jnp.where(is_target, logits, 0.0), axis=1)
        loss_sum = loss_sum + jnp.sum(wgt_rows * (log_norm - target))
        soft_probs = exp_shift / sum_exp[:, None]
        grad_logits = ((soft_probs - is_target.astype(jnp.float32)) * (wgt_rows / token_count)[:, None]).astype(jnp.bfloat16)
        d_rows = jnp.dot(grad_logits, w_vocab, preferred_element_type=jnp.float32).astype(jnp.bfloat16)
        dw_acc = dw_acc + lax.dot_general(grad_logits, hid_rows, (((0,), (0,)), ((), ())), preferred_element_type=jnp.float32)
        return (loss_sum, dw_acc), d_rows

    init = (jnp.zeros((), jnp.float32), jnp.zeros((VOCAB_SIZE, MODEL_DIM), jnp.float32))
    (loss_sum, dw_acc), dh_blocks = lax.scan(step, init, (hid_blocks, lab_blocks, wgt_blocks))
    d_hidden = dh_blocks.reshape(NUM_TOKENS, MODEL_DIM)
    return loss_sum / token_count, d_hidden, dw_acc.astype(jnp.bfloat16)
```

```python
import functools

import jax
import jax.numpy as jnp
from jax import lax
from jax.experimental import pallas as pl
from jax.experimental.pallas import tpu as pltpu
from jax.sharding import PartitionSpec as P


TOK, VOC, DIM, TM, LANE = 8192, 3144, 2560, 256, 128
NCH = 512
NEG = -3.0e38
AXES = ("data", "model")
MESH_ID = pl.DeviceIdType.MESH


def pairs(move):
    out = []
    for j in range(4):
        for k in range(4):
            z, y, x, c = move(j // 2, j % 2, k // 2, k % 2)
            out.append((j * 4 + k, (z * 2 + y) * 4 + x * 2 + c))
    return out


def role(x, c):
    return (x + 1 - c) % 2


TO_CORE = pairs(lambda z, y, x, c: (z, y, x, 1 - c))
TO_X = pairs(lambda z, y, x, c: (z, y, 1 - x, c))
TO_Z = pairs(lambda z, y, x, c: (1 - z, y, x, c))
RS_FIRST = pairs(lambda z, y, x, c: (z, y, 1 - x, 1 - c) if role(x, c) == 0 else (z, 1 - y, x, c))
RS_THIRD = pairs(lambda z, y, x, c: (z, y, 1 - x, 1 - c) if role(x, c) == 1 else (z, 1 - y, x, c))


def fwd_kernel(h_hbm, w_ref, lab_ref, z_ref, st_ref, hcat, buf, load_sem, store_sem, send_sem, recv_sem):
    i = pl.program_id(0)
    steps = pl.num_programs(0)
    j, k = lax.axis_index("data"), lax.axis_index("model")
    z, y, x, c = j // 2, j % 2, k // 2, k % 2
    b = (x + 1 - c) % 2
    yp = (z * 2 + 1 - y, k)
    zp = ((1 - z) * 2 + y, k)
    xp = (j, (1 - x) * 2 + c)
    sib = (j, x * 2 + 1 - c)
    first = ((z + c * (1 - 2 * z)) * 2 + y + (1 - c) * (1 - 2 * y), k)
    second = ((z + (1 - c) * (1 - 2 * z)) * 2 + y + c * (1 - 2 * y), k)

    def rows(tile):
        return pl.ds(pl.multiple_of(tile * TM, TM), TM)

    def slot(q, s):
        return hcat.at[rows(8 + q * 6 + s)]

    def remote(src, q, s, target):
        return pltpu.make_async_remote_copy(src_ref=src, dst_ref=slot(q, s), send_sem=send_sem.at[q, s], recv_sem=recv_sem.at[q, s], device_id=target, device_id_type=MESH_ID)

    def piece(q, s):
        src = [h_hbm.at[rows(b * 4 + q)], slot(q, 0), slot(q, 0), slot(q, 2), slot(q, 0), slot(q, 4)][s]
        return remote(src, q, s, [first, sib, second, sib, xp, sib][s])

    def load(tile_src, par):
        return pltpu.make_async_copy(tile_src, buf.at[par], load_sem.at[par])

    @pl.when(i == 0)
    def _():
        barrier = pltpu.get_barrier_semaphore()
        for target in (yp, zp, xp, sib):
            pl.semaphore_signal(barrier, inc=1, device_id=target, device_id_type=MESH_ID)
        load(h_hbm.at[rows(0)], 0).start()
        pl.semaphore_wait(barrier, 4)
        for q in range(4):
            piece(q, 0).start()

    @pl.when((i >= 3) & (i < 23) & ((i - 3) % 5 == 0))
    def _():
        q = (i - 3) // 5
        piece(q, 0).wait_recv()
        piece(q, 4).start()
        piece(q, 2).start()
        piece(q, 1).start()

    @pl.when((i >= 8) & (i < 28) & ((i - 8) % 5 == 0))
    def _():
        q = (i - 8) // 5
        piece(q, 2).wait_recv()
        piece(q, 3).start()
        piece(q, 4).wait_recv()
        piece(q, 5).start()

    par = i % 2
    load(h_hbm.at[rows(0)], par).wait()

    @pl.when((i > 0) & (i <= 8))
    def _():
        pltpu.make_async_copy(buf.at[1 - par], hcat.at[rows(0)], store_sem.at[1 - par]).wait()

    nxt = i + 1

    @pl.when(nxt < 8)
    def _():
        load(h_hbm.at[rows(nxt)], 1 - par).start()

    @pl.when((nxt >= 8) & (nxt < steps))
    def _():
        q, s = (nxt - 8) // 6, (nxt - 8) % 6
        for odd in (1, 3, 5):
            @pl.when(s == odd)
            def _():
                piece(q, odd).wait_recv()
        load(hcat.at[rows(nxt)], 1 - par).start()

    h = buf.at[par]
    lab = lab_ref[:, 0:1]
    m = jnp.full((TM, LANE), NEG, jnp.float32)
    s = jnp.zeros((TM, LANE), jnp.float32)
    t = jnp.zeros((TM, LANE), jnp.float32)
    lane = lax.broadcasted_iota(jnp.int32, (TM, LANE), 1)
    rel = lab - lane
    for n0 in range(0, VOC, NCH):
        n1 = min(n0 + NCH, VOC)
        logits = lax.dot_general(h[...], w_ref[n0:n1, :], (((1,), (1,)), ((), ())), preferred_element_type=jnp.float32)
        z_ref[:, n0:n1] = logits
        cols = []
        for g in range(n0, n1, LANE):
            wd = min(LANE, n1 - g)
            col = logits[:, g - n0:g - n0 + wd]
            if wd < LANE:
                col = jnp.concatenate([col, jnp.full((TM, LANE - wd), NEG, jnp.float32)], axis=1)
            cols.append((g, col))
        top = m
        for g, col in cols:
            top = jnp.maximum(top, col)
        s = s * jnp.exp(m - top)
        for g, col in cols:
            s = s + jnp.exp(col - top)
            hit = (rel == g) if g + LANE <= VOC else (rel == g) & (lane < VOC - g)
            t = t + jnp.where(hit, col, 0.0)
        m = top
    mm = jnp.max(m, axis=1, keepdims=True)
    ss = jnp.sum(s * jnp.exp(m - mm), axis=1, keepdims=True)
    tt = jnp.sum(t, axis=1, keepdims=True)
    st_ref[...] = jnp.where(lane == 0, mm, jnp.where(lane == 1, ss, tt))

    @pl.when(i < 8)
    def _():
        pltpu.make_async_copy(buf.at[par], hcat.at[rows(i)], store_sem.at[par]).start()

    @pl.when(i == steps - 1)
    def _():
        for q in range(4):
            for kind in range(6):
                piece(q, kind).wait_send()


def forward(hidden, w, lab):
    steps = TOK // TM
    return pl.pallas_call(
        fwd_kernel,
        out_shape=[jax.ShapeDtypeStruct((TOK, VOC), jnp.float32), jax.ShapeDtypeStruct((TOK, LANE), jnp.float32), jax.ShapeDtypeStruct((TOK, DIM), jnp.bfloat16)],
        grid=(steps,),
        in_specs=[pl.BlockSpec(memory_space=pl.ANY), pl.BlockSpec((VOC, DIM), lambda i: (0, 0), pipeline_mode=pl.Buffered(1)), pl.BlockSpec((TM, LANE), lambda i: (i, 0))],
        out_specs=[pl.BlockSpec((TM, VOC), lambda i: (i, 0)), pl.BlockSpec((TM, LANE), lambda i: (i, 0)), pl.BlockSpec(memory_space=pl.ANY)],
        scratch_shapes=[pltpu.VMEM((2, TM, DIM), jnp.bfloat16), pltpu.SemaphoreType.DMA((2,)), pltpu.SemaphoreType.DMA((2,)), pltpu.SemaphoreType.DMA((4, 6)), pltpu.SemaphoreType.DMA((4, 6))],
        compiler_params=pltpu.CompilerParams(dimension_semantics=("arbitrary",), collective_id=0, has_side_effects=True, vmem_limit_bytes=60 * 2**20),
        cost_estimate=pl.CostEstimate(flops=2 * TOK * VOC * DIM, bytes_accessed=TOK * (VOC * 4 + DIM * 4) + VOC * DIM * 2, transcendentals=TOK * VOC),
    )(hidden, w, lab)


def stats_kernel(x_ref, lse_ref, tgt_ref, got, send_sem, recv_sem):
    me = lax.axis_index("data") * 4 + lax.axis_index("model")
    barrier = pltpu.get_barrier_semaphore()
    peers = []
    for r in range(1, 16):
        p = (me + r) % 16
        peers.append((p // 4, p % 4))
        pl.semaphore_signal(barrier, inc=1, device_id=peers[-1], device_id_type=MESH_ID)
    pl.semaphore_wait(barrier, 15)
    copies = [pltpu.make_async_remote_copy(src_ref=x_ref, dst_ref=got.at[r], send_sem=send_sem.at[r], recv_sem=recv_sem.at[r], device_id=peers[r], device_id_type=MESH_ID) for r in range(15)]
    for copy in copies:
        copy.start()
    for copy in copies:
        copy.wait_recv()
    top = x_ref[0]
    for r in range(15):
        top = jnp.maximum(top, got[r, 0])
    total = x_ref[1] * jnp.exp(x_ref[0] - top)
    tgt = x_ref[2]
    for r in range(15):
        total = total + got[r, 1] * jnp.exp(got[r, 0] - top)
        tgt = tgt + got[r, 2]
    lse_ref[...] = top + jnp.log(total)
    tgt_ref[...] = tgt
    for copy in copies:
        copy.wait_send()


def combine(parts):
    return pl.pallas_call(
        stats_kernel,
        out_shape=[jax.ShapeDtypeStruct((32, TM), jnp.float32)] * 2,
        in_specs=[pl.BlockSpec(memory_space=pltpu.VMEM)],
        out_specs=[pl.BlockSpec(memory_space=pltpu.VMEM)] * 2,
        scratch_shapes=[pltpu.VMEM((15, 3, 32, TM), jnp.float32), pltpu.SemaphoreType.DMA((15,)), pltpu.SemaphoreType.DMA((15,))],
        compiler_params=pltpu.CompilerParams(collective_id=1, has_side_effects=True),
    )(parts)


HT = 128


def bwd_tile(z_ref, info_ref, w_ref, recv_ref, out_ref, g_ref):
    info = info_ref[...]
    lse, scale, lab = info[:, 0:1], info[:, 1:2], info[:, 2:3]
    rel = lab - lax.broadcasted_iota(jnp.int32, (HT, LANE), 1).astype(jnp.float32)
    for g in range(0, VOC, LANE):
        wd = min(LANE, VOC - g)
        p = jnp.exp(z_ref[:, g:g + wd] - lse)
        g_ref[:, g:g + wd] = ((p - jnp.where(rel[:, :wd] == float(g), 1.0, 0.0)) * scale).astype(jnp.bfloat16)
    for n in range(0, DIM, NCH):
        o = jnp.dot(g_ref[...], w_ref[:, n:n + NCH], preferred_element_type=jnp.float32)
        if recv_ref is not None:
            o = o + recv_ref[:, n:n + NCH]
        out_ref[:, n:n + NCH] = o


def bwd_kernel(idx, *refs, has_recv, has_g):
    refs = list(refs)
    z_ref, info_ref, w_ref = refs[:3]
    recv_ref = refs[3] if has_recv else None
    outs = refs[3 + has_recv + has_g:]
    if not has_recv:
        bwd_tile(z_ref, info_ref, w_ref, None, outs[0], outs[1])
        return
    i, half = pl.program_id(0), pl.num_programs(0) // 2

    @pl.when(i < half)
    def _():
        bwd_tile(z_ref, info_ref, w_ref, recv_ref, outs[0], outs[2])

    @pl.when(i >= half)
    def _():
        bwd_tile(z_ref, info_ref, w_ref, recv_ref, outs[1], outs[2])


def backward(idx, z, info, w, g, recv):
    tiles = idx.shape[0]
    n = tiles * HT
    row = lambda i, ix: (ix[i], 0)
    seq = lambda i, ix: (i, 0)
    specs = [pl.BlockSpec((HT, VOC), row), pl.BlockSpec((HT, LANE), row), pl.BlockSpec((VOC, DIM), lambda i, ix: (0, 0), pipeline_mode=pl.Buffered(1))]
    args = [z, info, w]
    if recv is not None:
        specs.append(pl.BlockSpec((HT, DIM), seq))
        args.append(recv)
        half = tiles // 2
        outs = [jax.ShapeDtypeStruct((n // 2, DIM), jnp.float32)] * 2
        ospecs = [pl.BlockSpec((HT, DIM), lambda i, ix: (jnp.minimum(i, half - 1), 0)), pl.BlockSpec((HT, DIM), lambda i, ix: (jnp.maximum(i - half, 0), 0))]
    else:
        outs, ospecs = [jax.ShapeDtypeStruct((n, DIM), jnp.float32)], [pl.BlockSpec((HT, DIM), seq)]
    alias = {}
    if g is not None:
        specs.append(pl.BlockSpec(memory_space=pl.ANY))
        args.append(g)
        alias = {len(args): len(outs)}
    outs = outs + [jax.ShapeDtypeStruct((TOK, VOC), jnp.bfloat16)]
    ospecs = ospecs + [pl.BlockSpec((HT, VOC), row)]
    return pl.pallas_call(
        functools.partial(bwd_kernel, has_recv=recv is not None, has_g=g is not None),
        out_shape=outs,
        grid_spec=pltpu.PrefetchScalarGridSpec(num_scalar_prefetch=1, grid=(tiles,), in_specs=specs, out_specs=ospecs),
        input_output_aliases=alias,
        compiler_params=pltpu.CompilerParams(dimension_semantics=("arbitrary",), vmem_limit_bytes=60 * 2**20),
        cost_estimate=pl.CostEstimate(flops=2 * n * VOC * DIM, bytes_accessed=n * (VOC * 6 + DIM * 8) + VOC * DIM * 2, transcendentals=n * VOC),
    )(idx, *args)


def solution(mesh):
    def local_step(hidden, w, labels, mask):
        j, k = lax.axis_index("data"), lax.axis_index("model")
        x, c = k // 2, k % 2
        b = (x + 1 - c) % 2
        i32 = lambda *v: jnp.stack([jnp.asarray(u, jnp.int32) for u in v])

        own = jnp.arange(8, dtype=jnp.int32)
        shard_a, shard_b, shard_d = j ^ (1 + c), j ^ (2 - c), j ^ 3
        q4 = jnp.arange(4, dtype=jnp.int32)[:, None]
        base = i32(shard_a * 8 + b * 4, shard_b * 8 + (1 - b) * 4, shard_d * 8 + b * 4, shard_d * 8 + (1 - b) * 4, shard_a * 8 + (1 - b) * 4, shard_b * 8 + b * 4)
        tiles = jnp.concatenate([j * 8 + own, (base[None, :] + q4).reshape(24)])
        place = tiles[:, None] == jnp.arange(32, dtype=jnp.int32)[None, :]

        def held(v):
            return jnp.sum(jnp.where(place[:, :, None], v[None], jnp.zeros((), v.dtype)), axis=1, dtype=v.dtype)

        def whole(v):
            return jnp.sum(jnp.where(place[:, :, None], v[:, None], jnp.zeros((), v.dtype)), axis=0, dtype=v.dtype)

        both = lax.all_gather(jnp.stack([labels, mask]), "data")
        lab_all = both[:, 0].reshape(32, TM)
        weight = both[:, 1].reshape(32, TM).astype(jnp.float32)
        count = jnp.sum(weight)
        local = held(lab_all - (k * 12576 + j * VOC)).reshape(TOK)

        z, stats, h_all = forward(hidden, w, jnp.broadcast_to(local[:, None], (TOK, LANE)))

        lse, target = combine(jnp.stack([whole(stats[:, n].reshape(32, TM)) for n in range(3)]))
        loss = jnp.sum(weight * (lse - target)) / count
        info = jnp.stack([held(lse).reshape(TOK), held(weight / count).reshape(TOK), local.astype(jnp.float32)], axis=1)
        info = jnp.pad(info, ((0, 0), (0, LANE - 3)))

        def order(q, bb, sections):
            def at(sec, dx):
                return sections[sec] * 2 + (x + dx) % 2
            r0 = i32(at(0, 1), at(1, 1), at(2, 1), at(3, 1), at(0, 0), at(1, 0), at(2, 0), at(3, 0))
            r1 = i32(at(1, 0), at(1, 1), at(3, 0), at(3, 1), at(0, 0), at(0, 1), at(2, 0), at(2, 1))
            return jnp.where(bb == 0, r0, r1)

        def keep_order(q):
            d1, d2, e3 = 8 + q * 6, 8 + q * 6 + 2, 8 + q * 6 + 5
            return order(q, b, [b * 4 + q, jnp.where(c == 0, d1, e3), jnp.where(c == 0, e3, d1), d2])

        def send_order(q):
            d3, e1, e2 = 8 + q * 6 + 4, 8 + q * 6 + 1, 8 + q * 6 + 3
            return order(q, 1 - b, [(1 - b) * 4 + q, jnp.where(c == 0, d3, e1), jnp.where(c == 0, e1, d3), e2])

        g = None
        recv, parts, finals = {}, [], []
        def do_send(q, g):
            out, g = backward(send_order(q), z, info, w, g, None)
            recv[q] = lax.ppermute(out, AXES, TO_CORE)
            return g
        g = do_send(0, g)
        for q in range(4):
            if q < 3:
                g = do_send(q + 1, g)
            s1, k1, g = backward(keep_order(q), z, info, w, g, recv[q])
            r1 = lax.ppermute(s1, AXES, RS_FIRST)
            r2 = lax.ppermute(k1[256:] + r1[256:], AXES, TO_Z)
            r3 = lax.ppermute(k1[128:256] + r1[128:256] + r2[128:], AXES, RS_THIRD)
            finals.append((k1[:128] + r1[:128] + r2[:128] + r3).astype(jnp.bfloat16))

        cuts = [0, 768, 1536, 2304, VOC]
        d_w = jnp.concatenate([lax.dot_general(g[:, a:e], h_all, (((0,), (0,)), ((), ())), preferred_element_type=jnp.float32).astype(jnp.bfloat16) for a, e in zip(cuts, cuts[1:])], axis=0)

        mine = jnp.stack(finals)
        theirs = lax.ppermute(mine, AXES, TO_CORE)
        mine_x = lax.ppermute(mine, AXES, TO_X)
        theirs_x = lax.ppermute(mine_x, AXES, TO_CORE)
        d_hidden = jnp.zeros((2, 4, 2, HT, DIM), jnp.bfloat16)
        for half, side, block in ((b, x, mine), (1 - b, x, theirs), (1 - b, 1 - x, mine_x), (b, 1 - x, theirs_x)):
            d_hidden = lax.dynamic_update_slice(d_hidden, block[None, :, None], (half, 0, side, 0, 0))
        d_hidden = d_hidden.reshape(2048, DIM)
        return loss, d_hidden, d_w

    return jax.shard_map(local_step, mesh=mesh, in_specs=(P("data", None), P(("model", "data"), None), P("data"), P("data")), out_specs=(P(), P("data", None), P(("model", "data"), None)), check_vma=False)
```

```python
import functools

import jax
import jax.numpy as jnp
from jax import lax
from jax.experimental import pallas as pl
from jax.experimental.pallas import tpu as pltpu
from jax.sharding import PartitionSpec as P


TOK, VOC, DIM, TM, LANE = 8192, 3144, 2560, 256, 128
NCH = 512
NEG = -3.0e38
AXES = ("data", "model")
MESH_ID = pl.DeviceIdType.MESH


def pairs(move):
    out = []
    for j in range(4):
        for k in range(4):
            z, y, x, c = move(j // 2, j % 2, k // 2, k % 2)
            out.append((j * 4 + k, (z * 2 + y) * 4 + x * 2 + c))
    return out


def role(x, c):
    return (x + 1 - c) % 2


TO_CORE = pairs(lambda z, y, x, c: (z, y, x, 1 - c))
TO_X = pairs(lambda z, y, x, c: (z, y, 1 - x, c))
TO_Z = pairs(lambda z, y, x, c: (1 - z, y, x, c))
RS_FIRST = pairs(lambda z, y, x, c: (z, y, 1 - x, 1 - c) if role(x, c) == 0 else (z, 1 - y, x, c))
RS_THIRD = pairs(lambda z, y, x, c: (z, y, 1 - x, 1 - c) if role(x, c) == 1 else (z, 1 - y, x, c))


def fwd_kernel(h_hbm, w_ref, lab_ref, z_ref, st_ref, hcat, buf, load_sem, store_sem, send_sem, recv_sem):
    i = pl.program_id(0)
    steps = pl.num_programs(0)
    j, k = lax.axis_index("data"), lax.axis_index("model")
    z, y, x, c = j // 2, j % 2, k // 2, k % 2
    b = (x + 1 - c) % 2
    yp = (z * 2 + 1 - y, k)
    zp = ((1 - z) * 2 + y, k)
    xp = (j, (1 - x) * 2 + c)
    sib = (j, x * 2 + 1 - c)
    first = ((z + c * (1 - 2 * z)) * 2 + y + (1 - c) * (1 - 2 * y), k)
    second = ((z + (1 - c) * (1 - 2 * z)) * 2 + y + c * (1 - 2 * y), k)

    def rows(tile):
        return pl.ds(pl.multiple_of(tile * TM, TM), TM)

    def slot(q, s):
        return hcat.at[rows(8 + q * 6 + s)]

    def remote(src, q, s, target):
        return pltpu.make_async_remote_copy(src_ref=src, dst_ref=slot(q, s), send_sem=send_sem.at[q, s], recv_sem=recv_sem.at[q, s], device_id=target, device_id_type=MESH_ID)

    def piece(q, s):
        src = [h_hbm.at[rows(b * 4 + q)], slot(q, 0), slot(q, 0), slot(q, 2), slot(q, 0), slot(q, 4)][s]
        return remote(src, q, s, [first, sib, second, sib, xp, sib][s])

    def load(tile_src, par):
        return pltpu.make_async_copy(tile_src, buf.at[par], load_sem.at[par])

    @pl.when(i == 0)
    def _():
        barrier = pltpu.get_barrier_semaphore()
        for target in (yp, zp, xp, sib):
            pl.semaphore_signal(barrier, inc=1, device_id=target, device_id_type=MESH_ID)
        load(h_hbm.at[rows(0)], 0).start()
        pl.semaphore_wait(barrier, 4)
        for q in range(4):
            piece(q, 0).start()

    @pl.when((i >= 3) & (i < 23) & ((i - 3) % 5 == 0))
    def _():
        q = (i - 3) // 5
        piece(q, 0).wait_recv()
        piece(q, 4).start()
        piece(q, 2).start()
        piece(q, 1).start()

    @pl.when((i >= 8) & (i < 28) & ((i - 8) % 5 == 0))
    def _():
        q = (i - 8) // 5
        piece(q, 2).wait_recv()
        piece(q, 3).start()
        piece(q, 4).wait_recv()
        piece(q, 5).start()

    par = i % 2
    load(h_hbm.at[rows(0)], par).wait()

    @pl.when((i > 0) & (i <= 8))
    def _():
        pltpu.make_async_copy(buf.at[1 - par], hcat.at[rows(0)], store_sem.at[1 - par]).wait()

    nxt = i + 1

    @pl.when(nxt < 8)
    def _():
        load(h_hbm.at[rows(nxt)], 1 - par).start()

    @pl.when((nxt >= 8) & (nxt < steps))
    def _():
        q, s = (nxt - 8) // 6, (nxt - 8) % 6
        for odd in (1, 3, 5):
            @pl.when(s == odd)
            def _():
                piece(q, odd).wait_recv()
        load(hcat.at[rows(nxt)], 1 - par).start()

    h = buf.at[par]
    lab = lab_ref[:, 0:1]
    m = jnp.full((TM, LANE), NEG, jnp.float32)
    s = jnp.zeros((TM, LANE), jnp.float32)
    t = jnp.zeros((TM, LANE), jnp.float32)
    lane = lax.broadcasted_iota(jnp.int32, (TM, LANE), 1)
    rel = lab - lane
    for n0 in range(0, VOC, NCH):
        n1 = min(n0 + NCH, VOC)
        logits = lax.dot_general(h[...], w_ref[n0:n1, :], (((1,), (1,)), ((), ())), preferred_element_type=jnp.float32)
        z_ref[:, n0:n1] = logits
        cols = []
        for g in range(n0, n1, LANE):
            wd = min(LANE, n1 - g)
            col = logits[:, g - n0:g - n0 + wd]
            if wd < LANE:
                col = jnp.concatenate([col, jnp.full((TM, LANE - wd), NEG, jnp.float32)], axis=1)
            cols.append((g, col))
        top = m
        for g, col in cols:
            top = jnp.maximum(top, col)
        s = s * jnp.exp(m - top)
        for g, col in cols:
            s = s + jnp.exp(col - top)
            hit = (rel == g) if g + LANE <= VOC else (rel == g) & (lane < VOC - g)
            t = t + jnp.where(hit, col, 0.0)
        m = top
    mm = jnp.max(m, axis=1, keepdims=True)
    ss = jnp.sum(s * jnp.exp(m - mm), axis=1, keepdims=True)
    tt = jnp.sum(t, axis=1, keepdims=True)
    st_ref[...] = jnp.where(lane == 0, mm, jnp.where(lane == 1, ss, tt))

    @pl.when(i < 8)
    def _():
        pltpu.make_async_copy(buf.at[par], hcat.at[rows(i)], store_sem.at[par]).start()

    @pl.when(i == steps - 1)
    def _():
        for q in range(4):
            for kind in range(6):
                piece(q, kind).wait_send()


def forward(hidden, w, lab):
    steps = TOK // TM
    return pl.pallas_call(
        fwd_kernel,
        out_shape=[jax.ShapeDtypeStruct((TOK, VOC), jnp.float32), jax.ShapeDtypeStruct((TOK, LANE), jnp.float32), jax.ShapeDtypeStruct((TOK, DIM), jnp.bfloat16)],
        grid=(steps,),
        in_specs=[pl.BlockSpec(memory_space=pl.ANY), pl.BlockSpec((VOC, DIM), lambda i: (0, 0), pipeline_mode=pl.Buffered(1)), pl.BlockSpec((TM, LANE), lambda i: (i, 0))],
        out_specs=[pl.BlockSpec((TM, VOC), lambda i: (i, 0)), pl.BlockSpec((TM, LANE), lambda i: (i, 0)), pl.BlockSpec(memory_space=pl.ANY)],
        scratch_shapes=[pltpu.VMEM((2, TM, DIM), jnp.bfloat16), pltpu.SemaphoreType.DMA((2,)), pltpu.SemaphoreType.DMA((2,)), pltpu.SemaphoreType.DMA((4, 6)), pltpu.SemaphoreType.DMA((4, 6))],
        compiler_params=pltpu.CompilerParams(dimension_semantics=("arbitrary",), collective_id=0, has_side_effects=True, vmem_limit_bytes=60 * 2**20),
        cost_estimate=pl.CostEstimate(flops=2 * TOK * VOC * DIM, bytes_accessed=TOK * (VOC * 4 + DIM * 4) + VOC * DIM * 2, transcendentals=TOK * VOC),
    )(hidden, w, lab)


def stats_kernel(x_ref, lse_ref, tgt_ref, got, send_sem, recv_sem):
    me = lax.axis_index("data") * 4 + lax.axis_index("model")
    barrier = pltpu.get_barrier_semaphore()
    peers = []
    for r in range(1, 16):
        p = (me + r) % 16
        peers.append((p // 4, p % 4))
        pl.semaphore_signal(barrier, inc=1, device_id=peers[-1], device_id_type=MESH_ID)
    pl.semaphore_wait(barrier, 15)
    copies = [pltpu.make_async_remote_copy(src_ref=x_ref, dst_ref=got.at[r], send_sem=send_sem.at[r], recv_sem=recv_sem.at[r], device_id=peers[r], device_id_type=MESH_ID) for r in range(15)]
    for copy in copies:
        copy.start()
    for copy in copies:
        copy.wait_recv()
    top = x_ref[0]
    for r in range(15):
        top = jnp.maximum(top, got[r, 0])
    total = x_ref[1] * jnp.exp(x_ref[0] - top)
    tgt = x_ref[2]
    for r in range(15):
        total = total + got[r, 1] * jnp.exp(got[r, 0] - top)
        tgt = tgt + got[r, 2]
    lse_ref[...] = top + jnp.log(total)
    tgt_ref[...] = tgt
    for copy in copies:
        copy.wait_send()


def combine(parts):
    return pl.pallas_call(
        stats_kernel,
        out_shape=[jax.ShapeDtypeStruct((32, TM), jnp.float32)] * 2,
        in_specs=[pl.BlockSpec(memory_space=pltpu.VMEM)],
        out_specs=[pl.BlockSpec(memory_space=pltpu.VMEM)] * 2,
        scratch_shapes=[pltpu.VMEM((15, 3, 32, TM), jnp.float32), pltpu.SemaphoreType.DMA((15,)), pltpu.SemaphoreType.DMA((15,))],
        compiler_params=pltpu.CompilerParams(collective_id=1, has_side_effects=True),
    )(parts)


HT = 128


def bwd_tile(z_ref, info_ref, w_ref, recv_ref, out_ref, g_ref):
    info = info_ref[...]
    lse, scale, lab = info[:, 0:1], info[:, 1:2], info[:, 2:3]
    rel = lab - lax.broadcasted_iota(jnp.int32, (HT, LANE), 1).astype(jnp.float32)
    for g in range(0, VOC, LANE):
        wd = min(LANE, VOC - g)
        p = jnp.exp(z_ref[:, g:g + wd] - lse)
        g_ref[:, g:g + wd] = ((p - jnp.where(rel[:, :wd] == float(g), 1.0, 0.0)) * scale).astype(jnp.bfloat16)
    for n in range(0, DIM, NCH):
        o = jnp.dot(g_ref[...], w_ref[:, n:n + NCH], preferred_element_type=jnp.float32)
        if recv_ref is not None:
            o = o + recv_ref[:, n:n + NCH]
        out_ref[:, n:n + NCH] = o


def bwd_kernel(idx, *refs, has_recv, has_g):
    refs = list(refs)
    z_ref, info_ref, w_ref = refs[:3]
    recv_ref = refs[3] if has_recv else None
    outs = refs[3 + has_recv + has_g:]
    if not has_recv:
        bwd_tile(z_ref, info_ref, w_ref, None, outs[0], outs[1])
        return
    i, half = pl.program_id(0), pl.num_programs(0) // 2

    @pl.when(i < half)
    def _():
        bwd_tile(z_ref, info_ref, w_ref, recv_ref, outs[0], outs[2])

    @pl.when(i >= half)
    def _():
        bwd_tile(z_ref, info_ref, w_ref, recv_ref, outs[1], outs[2])


def backward(idx, z, info, w, g, recv):
    tiles = idx.shape[0]
    n = tiles * HT
    row = lambda i, ix: (ix[i], 0)
    seq = lambda i, ix: (i, 0)
    specs = [pl.BlockSpec((HT, VOC), row), pl.BlockSpec((HT, LANE), row), pl.BlockSpec((VOC, DIM), lambda i, ix: (0, 0), pipeline_mode=pl.Buffered(1))]
    args = [z, info, w]
    if recv is not None:
        specs.append(pl.BlockSpec((HT, DIM), seq))
        args.append(recv)
        half = tiles // 2
        outs = [jax.ShapeDtypeStruct((n // 2, DIM), jnp.float32)] * 2
        ospecs = [pl.BlockSpec((HT, DIM), lambda i, ix: (jnp.minimum(i, half - 1), 0)), pl.BlockSpec((HT, DIM), lambda i, ix: (jnp.maximum(i - half, 0), 0))]
    else:
        outs, ospecs = [jax.ShapeDtypeStruct((n, DIM), jnp.float32)], [pl.BlockSpec((HT, DIM), seq)]
    alias = {}
    if g is not None:
        specs.append(pl.BlockSpec(memory_space=pl.ANY))
        args.append(g)
        alias = {len(args): len(outs)}
    outs = outs + [jax.ShapeDtypeStruct((TOK, VOC), jnp.bfloat16)]
    ospecs = ospecs + [pl.BlockSpec((HT, VOC), row)]
    return pl.pallas_call(
        functools.partial(bwd_kernel, has_recv=recv is not None, has_g=g is not None),
        out_shape=outs,
        grid_spec=pltpu.PrefetchScalarGridSpec(num_scalar_prefetch=1, grid=(tiles,), in_specs=specs, out_specs=ospecs),
        input_output_aliases=alias,
        compiler_params=pltpu.CompilerParams(dimension_semantics=("arbitrary",), vmem_limit_bytes=60 * 2**20),
        cost_estimate=pl.CostEstimate(flops=2 * n * VOC * DIM, bytes_accessed=n * (VOC * 6 + DIM * 8) + VOC * DIM * 2, transcendentals=n * VOC),
    )(idx, *args)


def solution(mesh):
    def local_step(hidden, w, labels, mask):
        j, k = lax.axis_index("data"), lax.axis_index("model")
        x, c = k // 2, k % 2
        b = (x + 1 - c) % 2
        i32 = lambda *v: jnp.stack([jnp.asarray(u, jnp.int32) for u in v])

        own = jnp.arange(8, dtype=jnp.int32)
        shard_a, shard_b, shard_d = j ^ (1 + c), j ^ (2 - c), j ^ 3
        q4 = jnp.arange(4, dtype=jnp.int32)[:, None]
        base = i32(shard_a * 8 + b * 4, shard_b * 8 + (1 - b) * 4, shard_d * 8 + b * 4, shard_d * 8 + (1 - b) * 4, shard_a * 8 + (1 - b) * 4, shard_b * 8 + b * 4)
        tiles = jnp.concatenate([j * 8 + own, (base[None, :] + q4).reshape(24)])
        place = tiles[:, None] == jnp.arange(32, dtype=jnp.int32)[None, :]

        def held(v):
            return jnp.sum(jnp.where(place[:, :, None], v[None], jnp.zeros((), v.dtype)), axis=1, dtype=v.dtype)

        def whole(v):
            return jnp.sum(jnp.where(place[:, :, None], v[:, None], jnp.zeros((), v.dtype)), axis=0, dtype=v.dtype)

        both = lax.all_gather(jnp.stack([labels, mask]), "data")
        lab_all = both[:, 0].reshape(32, TM)
        weight = both[:, 1].reshape(32, TM).astype(jnp.float32)
        count = jnp.sum(weight)
        local = held(lab_all - (k * 12576 + j * VOC)).reshape(TOK)

        z, stats, h_all = forward(hidden, w, jnp.broadcast_to(local[:, None], (TOK, LANE)))

        lse, target = combine(jnp.stack([whole(stats[:, n].reshape(32, TM)) for n in range(3)]))
        loss = jnp.sum(weight * (lse - target)) / count
        info = jnp.stack([held(lse).reshape(TOK), held(weight / count).reshape(TOK), local.astype(jnp.float32)], axis=1)
        info = jnp.pad(info, ((0, 0), (0, LANE - 3)))

        def order(bb, blocks):
            r0 = i32(blocks[0][1], blocks[1][1], blocks[2][1], blocks[3][1], blocks[0][0], blocks[1][0], blocks[2][0], blocks[3][0])
            r1 = i32(blocks[1][0], blocks[1][1], blocks[3][0], blocks[3][1], blocks[0][0], blocks[0][1], blocks[2][0], blocks[2][1])
            return jnp.where(bb == 0, r0, r1)

        def blocks(q, half, kinds):
            out = []
            for kind in kinds:
                row = []
                for dx in (0, 1):
                    tile = ((x + dx) % 2) * 2 + q // 2
                    row.append((half * 4 + tile if kind is None else 8 + tile * 6 + kind) * 2 + q % 2)
                out.append(row)
            return out

        def keep_order(q):
            return order(b, blocks(q, b, [None, jnp.where(c == 0, 0, 5), jnp.where(c == 0, 5, 0), 2]))

        def send_order(q):
            return order(1 - b, blocks(q, 1 - b, [None, jnp.where(c == 0, 4, 1), jnp.where(c == 0, 1, 4), 3]))

        g = None
        recv, finals = {}, []

        def do_send(q, g):
            out, g = backward(send_order(q), z, info, w, g, None)
            recv[q] = lax.ppermute(out, AXES, TO_CORE)
            return g

        g = do_send(0, g)
        for q in range(4):
            if q < 3:
                g = do_send(q + 1, g)
            s1, k1, g = backward(keep_order(q), z, info, w, g, recv[q])
            r1 = lax.ppermute(s1, AXES, RS_FIRST)
            s2 = k1[256:] + r1[256:]
            r2 = lax.ppermute(s2, AXES, TO_Z)
            s3 = k1[128:256] + r1[128:256] + r2[128:]
            r3 = lax.ppermute(s3, AXES, RS_THIRD)
            finals.append((k1[:128] + r1[:128] + r2[:128] + r3).astype(jnp.bfloat16))

        cuts = [0, 768, 1536, 2304, VOC]
        d_w = []
        for lo, hi in zip(cuts, cuts[1:]):
            d_w.append(lax.dot_general(g[:, lo:hi], h_all, (((0,), (0,)), ((), ())), preferred_element_type=jnp.float32).astype(jnp.bfloat16))
        d_w = jnp.concatenate(d_w, axis=0)

        d_hidden = jnp.zeros((2, 2, 512, DIM), jnp.bfloat16)
        for at, part in ((0, jnp.concatenate(finals[:3])), (384, finals[3])):
            theirs = lax.ppermute(part, AXES, TO_CORE)
            part_x = lax.ppermute(part, AXES, TO_X)
            theirs_x = lax.ppermute(part_x, AXES, TO_CORE)
            for half, side, block in ((b, x, part), (1 - b, x, theirs), (1 - b, 1 - x, part_x), (b, 1 - x, theirs_x)):
                d_hidden = lax.dynamic_update_slice(d_hidden, block[None, None], (half, side, at, 0))
        d_hidden = d_hidden.reshape(2048, DIM)
        return loss, d_hidden, d_w

    return jax.shard_map(local_step, mesh=mesh, in_specs=(P("data", None), P(("model", "data"), None), P("data"), P("data")), out_specs=(P(), P("data", None), P(("model", "data"), None)), check_vma=False)
```
